64 devices in a mesh: dp: 8 (over x, y, core), tp: 8 (over z).
Axes of the slice: x: 2, y: 2, z: 8, core: 2. Of those that a mesh axis runs over, the one named last changes fastest.
The devices are a block of a 4x4x8 slice.
Arguments:
- x: bfloat16 [16384, 4096], P(('dp', 'tp')), parts along dimension 0
- w_gate: bfloat16 [4096, 14336], P(None, 'tp')
- w_up: bfloat16 [4096, 14336], P(None, 'tp')
- w_down: bfloat16 [14336, 4096], P('tp')
Outputs:
- output: bfloat16 [16384, 4096], P(('dp', 'tp')), parts along dimension 0
There are 8 independent parts. The reference program is written for one: setup_inputs(seed, part) draws one part's arguments, and reference() takes and returns one part's arrays. A program takes and returns all parts, laid end to end along the dimension named above; an argument that names none is the same for every part.
All inputs are finite; a program needn't handle non-finite values.
Results may differ from the reference program's by a relative error of at most 0.016.
Values are sent between devices in bfloat16 or wider.
A program may use at most 768 MiB of HBM per device.

```python
import jax
import jax.numpy as jnp

ROWS = 2048
D = 4096
FF = 14336


def setup_inputs(seed: int = 0, part: int = 0) -> dict:
    kx, kg, ku, kd = jax.random.split(jax.random.key(seed), 4)
    drawn = {
        "x": jax.random.normal(jax.random.fold_in(kx, part), (ROWS, D), jnp.float32),
        "w_gate": jax.random.normal(kg, (D, FF), jnp.float32) * D**-0.5,
        "w_up": jax.random.normal(ku, (D, FF), jnp.float32) * D**-0.5,
        "w_down": jax.random.normal(kd, (FF, D), jnp.float32) * FF**-0.5,
    }
    return {k: v.astype(jnp.bfloat16) for k, v in drawn.items()}


def reference(x, w_gate, w_up, w_down):
    gate = jnp.dot(x, w_gate, preferred_element_type=jnp.float32)
    up = jnp.dot(x, w_up, preferred_element_type=jnp.float32)
    hidden = (jax.nn.silu(gate) * up).astype(jnp.bfloat16)
    return jnp.dot(hidden, w_down, preferred_element_type=jnp.float32).astype(jnp.bfloat16)
```

```python
import functools

import jax
import jax.numpy as jnp
from jax import lax
from jax.experimental import pallas as pl
from jax.experimental.pallas import tpu as pltpu
from jax.sharding import PartitionSpec as P

MESH = pl.DeviceIdType.MESH
SUBS = 2


def _kernel(
    n,
    x_ref,
    wg_ref,
    wu_ref,
    wd_ref,
    y_ref,
    xg_ref,
    rs_ref,
    wg,
    wu,
    wd,
    hid,
    xbuf,
    sbuf,
    acc,
    ag_send,
    ag_recv,
    rs_send,
    rs_recv,
    w_sem,
    x_sem,
    y_sem,
):
    rows, _ = x_ref.shape
    hidden = wg.shape[1]
    cols = wd.shape[1]
    half = rows // 2
    piece = half // SUBS
    pair = 2 * piece
    batches = n - 1
    nt_h = 256
    nt_y = 512
    me = lax.axis_index("tp")
    right, left = lax.rem(me + 1, n), lax.rem(me + n - 1, n)

    weights = [
        pltpu.make_async_copy(src, dst, w_sem.at[i])
        for i, (src, dst) in enumerate(((wg_ref, wg), (wu_ref, wu), (wd_ref, wd)))
    ]
    own = pltpu.make_async_copy(x_ref, xbuf, x_sem.at[0])

    barrier = pltpu.get_barrier_semaphore()
    for neighbour in (left, right):
        pl.semaphore_signal(barrier, inc=1, device_id={"tp": neighbour}, device_id_type=MESH)
    pl.semaphore_wait(barrier, 2)

    def at(s, d):
        return pl.ds(s * pair + d * piece, piece)

    def gather(b, s, d, src):
        return pltpu.make_async_remote_copy(
            src_ref=src,
            dst_ref=xg_ref.at[b, at(s, d)],
            send_sem=ag_send.at[b, s, d],
            recv_sem=ag_recv.at[b, s, d],
            device_id={"tp": right if d == 0 else left},
            device_id_type=MESH,
        )

    def gather_own(b, s, d):
        start = (b if d == 0 else 1 - b) * half + s * piece
        return gather(b, s, d, x_ref.at[pl.ds(start, piece)])

    def gather_on(b, s, d):
        return gather(b + 2, s, d, xg_ref.at[b, at(s, d)])

    def reduce(b, s, d, slot):
        return pltpu.make_async_remote_copy(
            src_ref=sbuf.at[slot, pl.ds(d * piece, piece)],
            dst_ref=rs_ref.at[b, at(s, d)],
            send_sem=rs_send.at[b, s, d],
            recv_sem=rs_recv.at[b, s, d],
            device_id={"tp": left if d == 0 else right},
            device_id_type=MESH,
        )

    for b in range(2):
        for s in range(SUBS):
            for d in range(2):
                gather_own(b, s, d).start()
    own.start()
    for w in weights:
        w.start()

    def mlp_in(b):
        def step(i, carry):
            c = pl.ds(pl.multiple_of(i * nt_h, nt_h), nt_h)
            x = xbuf[...]
            gate = jnp.dot(x, wg[:, c], preferred_element_type=jnp.float32)
            up = jnp.dot(x, wu[:, c], preferred_element_type=jnp.float32)
            hid[b, :, c] = (jax.nn.silu(gate) * up).astype(jnp.bfloat16)
            return carry

        lax.fori_loop(0, hidden // nt_h, step, 0)

    own.wait()
    weights[0].wait()
    weights[1].wait()
    mlp_in(batches)

    def batch_in(b, forward):
        for s in range(SUBS):
            for d in range(2):
                gather(b, s, d, xg_ref.at[b, at(s, d)]).wait_recv()
                if forward:
                    gather_on(b, s, d).start()
            r = pl.ds(s * pair, pair)
            pltpu.make_async_copy(xg_ref.at[b, r], xbuf.at[r], x_sem.at[s]).start()
        for s in range(SUBS):
            r = pl.ds(s * pair, pair)
            pltpu.make_async_copy(xg_ref.at[b, r], xbuf.at[r], x_sem.at[s]).wait()
        mlp_in(b)

    def batch_out(b, s, slot, add):
        h = pl.ds(s * pair, pair)
        buf = pl.ds(s * pair, pair)
        if add:
            for d in range(2):
                reduce(b + 2, s, d, slot).wait_recv()
            got = pltpu.make_async_copy(rs_ref.at[b + 2, h], xbuf.at[buf], x_sem.at[s])
            got.start()
            got.wait()

        def step(i, carry):
            c = pl.ds(pl.multiple_of(i * nt_y, nt_y), nt_y)
            term = jnp.dot(hid[b, h, :], wd[:, c], preferred_element_type=jnp.float32)
            if add:
                term = term + xbuf[buf, c].astype(jnp.float32)
            sbuf[slot, :, c] = term.astype(jnp.bfloat16)
            return carry

        lax.fori_loop(0, cols // nt_y, step, 0)
        for d in range(2):
            reduce(b, s, d, slot).start()

    def in_only(b, carry):
        batch_in(b, True)
        return carry

    lax.fori_loop(0, batches - 2, in_only, 0)

    weights[2].wait()

    def in_out(i, carry):
        b = batches - 2 + i
        batch_in(b, False)
        for s in range(SUBS):
            batch_out(b, s, i * SUBS + s, False)
        return carry

    lax.fori_loop(0, 2, in_out, 0)

    def out_only(k, carry):
        i = lax.rem(k, 2)
        b = batches - 4 - 2 * (k // 2) + i
        for s in range(SUBS):
            slot = i * SUBS + s
            for d in range(2):
                reduce(b + 2, s, d, slot).wait_send()
            batch_out(b, s, slot, True)
        return carry

    lax.fori_loop(0, batches - 3, out_only, 0)

    def own_term(i, carry):
        c = pl.ds(pl.multiple_of(i * nt_y, nt_y), nt_y)
        acc[:, c] = jnp.dot(hid[batches], wd[:, c], preferred_element_type=jnp.float32)
        return carry

    lax.fori_loop(0, cols // nt_y, own_term, 0)

    for s in range(SUBS):
        for d in range(2):
            reduce(1, s, d, s).wait_send()
        batch_out(0, s, s, True)

    for t in (1, 0):
        for s in range(SUBS):
            for d in range(2):
                reduce(t, s, d, s).wait_recv()
            r = pl.ds(s * pair, pair)
            got = pltpu.make_async_copy(rs_ref.at[t, r], xbuf.at[r], x_sem.at[s])
            got.start()
            got.wait()
            for d in range(2):
                o = pl.ds((t if d == 0 else 1 - t) * half + s * piece, piece)
                total = acc[o, :] + xbuf[at(s, d), :].astype(jnp.float32)
                if t == 1:
                    acc[o, :] = total
                else:
                    slot = SUBS + s
                    if s == 0 and d == 0:
                        for e in range(2 * SUBS):
                            reduce(2, e // 2, e % 2, SUBS + e // 2).wait_send()
                    sbuf[slot, pl.ds(d * piece, piece), :] = total.astype(jnp.bfloat16)
                    pltpu.make_async_copy(
                        sbuf.at[slot, pl.ds(d * piece, piece)], y_ref.at[o], y_sem.at[s, d]
                    ).start()

    for s in range(SUBS):
        for d in range(2):
            for b in range(batches):
                gather(b, s, d, xg_ref.at[b, at(s, d)]).wait_send()
            reduce(0, s, d, s).wait_send()
            o = pl.ds((0 if d == 0 else 1) * half + s * piece, piece)
            pltpu.make_async_copy(
                sbuf.at[SUBS + s, pl.ds(d * piece, piece)], y_ref.at[o], y_sem.at[s, d]
            ).wait()


def solution(mesh):
    n = mesh.shape["tp"]

    def step(x, w_gate, w_up, w_down):
        rows, dim = x.shape
        hidden = w_gate.shape[1]
        batches = n - 1
        piece = rows // (2 * SUBS)
        flops = 6 * n * rows * dim * hidden
        wire = 2 * batches * rows * dim * 2
        any_space = pl.BlockSpec(memory_space=pltpu.MemorySpace.HBM)
        y, _, _ = pl.pallas_call(
            functools.partial(_kernel, n),
            out_shape=(
                jax.ShapeDtypeStruct((rows, dim), jnp.bfloat16),
                jax.ShapeDtypeStruct((batches, rows, dim), jnp.bfloat16),
                jax.ShapeDtypeStruct((batches, rows, dim), jnp.bfloat16),
            ),
            in_specs=[any_space] * 4,
            out_specs=(any_space,) * 3,
            scratch_shapes=[
                pltpu.VMEM(w_gate.shape, jnp.bfloat16),
                pltpu.VMEM(w_up.shape, jnp.bfloat16),
                pltpu.VMEM(w_down.shape, jnp.bfloat16),
                pltpu.VMEM((n, rows, hidden), jnp.bfloat16),
                pltpu.VMEM((rows, dim), jnp.bfloat16),
                pltpu.VMEM((2 * SUBS, 2 * piece, dim), jnp.bfloat16),
                pltpu.VMEM((rows, dim), jnp.float32),
                pltpu.SemaphoreType.DMA((batches, SUBS, 2)),
                pltpu.SemaphoreType.DMA((batches, SUBS, 2)),
                pltpu.SemaphoreType.DMA((batches, SUBS, 2)),
                pltpu.SemaphoreType.DMA((batches, SUBS, 2)),
                pltpu.SemaphoreType.DMA((3,)),
                pltpu.SemaphoreType.DMA((SUBS,)),
                pltpu.SemaphoreType.DMA((SUBS, 2)),
            ],
            compiler_params=pltpu.CompilerParams(
                collective_id=0, has_side_effects=True, vmem_limit_bytes=67043328
            ),
            cost_estimate=pl.CostEstimate(
                flops=flops, bytes_accessed=3 * w_gate.size * 2 + 4 * wire, transcendentals=n * rows * hidden
            ),
            name="mlp_ring",
        )(x, w_gate, w_up, w_down)
        return y

    return jax.shard_map(
        step,
        mesh=mesh,
        in_specs=(P(("dp", "tp"), None), P(None, "tp"), P(None, "tp"), P("tp", None)),
        out_specs=P(("dp", "tp"), None),
        check_vma=False,
    )
```

```python
import functools

import jax
import jax.numpy as jnp
from jax import lax
from jax.experimental import pallas as pl
from jax.experimental.pallas import tpu as pltpu
from jax.sharding import PartitionSpec as P

MESH = pl.DeviceIdType.MESH
VMEM_LIMIT = 60 * 2**20
SUBS = 2


def _kernel(
    n,
    x_ref,
    wg_ref,
    wu_ref,
    wd_ref,
    y_ref,
    xg_ref,
    rs_ref,
    wg,
    wu,
    wd,
    hid,
    xbuf,
    sbuf,
    acc,
    ag_send,
    ag_recv,
    rs_send,
    rs_recv,
    w_sem,
    x_sem,
):
    rows, _ = x_ref.shape
    hidden = wg.shape[1]
    cols = wd.shape[1]
    half = rows // 2
    piece = half // SUBS
    pair = 2 * piece
    batches = n - 1
    nt_h = 256
    nt_y = 512
    me = lax.axis_index("tp")
    right, left = lax.rem(me + 1, n), lax.rem(me + n - 1, n)

    weights = [
        pltpu.make_async_copy(src, dst, w_sem.at[i])
        for i, (src, dst) in enumerate(((wg_ref, wg), (wu_ref, wu), (wd_ref, wd)))
    ]
    own = pltpu.make_async_copy(x_ref, xbuf, x_sem.at[0])

    barrier = pltpu.get_barrier_semaphore()
    for neighbour in (left, right):
        pl.semaphore_signal(barrier, inc=1, device_id={"tp": neighbour}, device_id_type=MESH)
    pl.semaphore_wait(barrier, 2)

    def at(s, d):
        return pl.ds(s * pair + d * piece, piece)

    def gather(b, s, d, src):
        return pltpu.make_async_remote_copy(
            src_ref=src,
            dst_ref=xg_ref.at[b, at(s, d)],
            send_sem=ag_send.at[b, s, d],
            recv_sem=ag_recv.at[b, s, d],
            device_id={"tp": right if d == 0 else left},
            device_id_type=MESH,
        )

    def gather_own(b, s, d):
        start = (b if d == 0 else 1 - b) * half + s * piece
        return gather(b, s, d, x_ref.at[pl.ds(start, piece)])

    def gather_on(b, s, d):
        return gather(b + 2, s, d, xg_ref.at[b, at(s, d)])

    def home(t, s, d):
        return pl.ds((t if d == 0 else 1 - t) * half + s * piece, piece)

    def reduce(b, s, d, slot, last=False):
        return pltpu.make_async_remote_copy(
            src_ref=sbuf.at[slot, pl.ds(d * piece, piece)],
            dst_ref=y_ref.at[home(0, s, d)] if last else rs_ref.at[b - 1, at(s, d)],
            send_sem=rs_send.at[b, s, d],
            recv_sem=rs_recv.at[b, s, d],
            device_id={"tp": left if d == 0 else right},
            device_id_type=MESH,
        )

    for b in range(2):
        for s in range(SUBS):
            for d in range(2):
                gather_own(b, s, d).start()
    own.start()
    for w in weights:
        w.start()

    def mlp_in(b):
        def step(i, carry):
            c = pl.ds(pl.multiple_of(i * nt_h, nt_h), nt_h)
            x = xbuf[...]
            gate = jnp.dot(x, wg[:, c], preferred_element_type=jnp.float32)
            up = jnp.dot(x, wu[:, c], preferred_element_type=jnp.float32)
            hid[b, :, c] = (jax.nn.silu(gate) * up).astype(jnp.bfloat16)
            return carry

        lax.fori_loop(0, hidden // nt_h, step, 0)

    own.wait()
    weights[0].wait()
    weights[1].wait()
    mlp_in(0)
    weights[2].wait()

    def own_term(i, carry):
        c = pl.ds(pl.multiple_of(i * nt_y, nt_y), nt_y)
        acc[:, c] = jnp.dot(hid[0], wd[:, c], preferred_element_type=jnp.float32)
        return carry

    lax.fori_loop(0, cols // nt_y, own_term, 0)

    def batch_in(b, forward):
        for s in range(SUBS):
            for d in range(2):
                gather(b, s, d, xg_ref.at[b, at(s, d)]).wait_recv()
                if forward:
                    gather_on(b, s, d).start()
            r = pl.ds(s * pair, pair)
            pltpu.make_async_copy(xg_ref.at[b, r], xbuf.at[r], x_sem.at[s]).start()
        for s in range(SUBS):
            r = pl.ds(s * pair, pair)
            pltpu.make_async_copy(xg_ref.at[b, r], xbuf.at[r], x_sem.at[s]).wait()
        mlp_in(b)

    def batch_out(b, s, slot, add, last=False):
        h = pl.ds(s * pair, pair)
        buf = pl.ds(s * pair, pair)
        if add:
            for d in range(2):
                reduce(b + 2, s, d, slot).wait_recv()
            got = pltpu.make_async_copy(rs_ref.at[b + 1, h], xbuf.at[buf], x_sem.at[s])
            got.start()
            got.wait()

        def step(i, carry):
            c = pl.ds(pl.multiple_of(i * nt_y, nt_y), nt_y)
            term = jnp.dot(hid[b, h, :], wd[:, c], preferred_element_type=jnp.float32)
            if add:
                term = term + xbuf[buf, c].astype(jnp.float32)
            sbuf[slot, :, c] = term.astype(jnp.bfloat16)
            return carry

        lax.fori_loop(0, cols // nt_y, step, 0)
        for d in range(2):
            reduce(b, s, d, slot, last).start()

    def in_only(b, carry):
        batch_in(b, True)
        return carry

    lax.fori_loop(0, batches - 2, in_only, 0)

    def in_out(i, carry):
        b = batches - 2 + i
        batch_in(b, False)
        for s in range(SUBS):
            batch_out(b, s, i * SUBS + s, False)
        return carry

    lax.fori_loop(0, 2, in_out, 0)

    def out_only(k, carry):
        i = lax.rem(k, 2)
        b = batches - 4 - 2 * (k // 2) + i
        for s in range(SUBS):
            slot = i * SUBS + s
            for d in range(2):
                reduce(b + 2, s, d, slot).wait_send()
            batch_out(b, s, slot, True)
        return carry

    lax.fori_loop(0, batches - 3, out_only, 0)

    for s in range(SUBS):
        for d in range(2):
            reduce(1, s, d, s).wait_send()
        batch_out(0, s, s, True, last=True)

    for s in range(SUBS):
        for d in range(2):
            reduce(1, s, d, s).wait_recv()
        r = pl.ds(s * pair, pair)
        got = pltpu.make_async_copy(rs_ref.at[0, r], xbuf.at[r], x_sem.at[s])
        got.start()
        got.wait()
        for d in range(2):
            o = home(1, s, d)
            acc[o, :] = acc[o, :] + xbuf[at(s, d), :].astype(jnp.float32)

    for s in range(SUBS):
        for d in range(2):
            for b in range(batches):
                gather(b, s, d, xg_ref.at[b, at(s, d)]).wait_send()
            reduce(2, s, d, SUBS + s).wait_send()

    for s in range(SUBS):
        for d in range(2):
            reduce(0, s, d, s, last=True).wait_recv()
        for d in range(2):
            o = home(0, s, d)
            y_ref[o, :] = (acc[o, :] + y_ref[o, :].astype(jnp.float32)).astype(jnp.bfloat16)

    for s in range(SUBS):
        for d in range(2):
            reduce(0, s, d, s, last=True).wait_send()


def solution(mesh):
    n = mesh.shape["tp"]

    def step(x, w_gate, w_up, w_down):
        rows, dim = x.shape
        hidden = w_gate.shape[1]
        batches = n - 1
        piece = rows // (2 * SUBS)
        flops = 6 * n * rows * dim * hidden
        wire = 2 * batches * rows * dim * 2
        any_space = pl.BlockSpec(memory_space=pltpu.MemorySpace.HBM)
        y, _, _ = pl.pallas_call(
            functools.partial(_kernel, n),
            out_shape=(
                pltpu.VMEM((rows, dim), jnp.bfloat16),
                jax.ShapeDtypeStruct((batches, rows, dim), jnp.bfloat16),
                jax.ShapeDtypeStruct((batches - 1, rows, dim), jnp.bfloat16),
            ),
            in_specs=[any_space] * 4,
            out_specs=(pl.BlockSpec(memory_space=pltpu.MemorySpace.VMEM), any_space, any_space),
            scratch_shapes=[
                pltpu.VMEM(w_gate.shape, jnp.bfloat16),
                pltpu.VMEM(w_up.shape, jnp.bfloat16),
                pltpu.VMEM(w_down.shape, jnp.bfloat16),
                pltpu.VMEM((batches, rows, hidden), jnp.bfloat16),
                pltpu.VMEM((rows, dim), jnp.bfloat16),
                pltpu.VMEM((2 * SUBS, 2 * piece, dim), jnp.bfloat16),
                pltpu.VMEM((rows, dim), jnp.float32),
                pltpu.SemaphoreType.DMA((batches, SUBS, 2)),
                pltpu.SemaphoreType.DMA((batches, SUBS, 2)),
                pltpu.SemaphoreType.DMA((batches, SUBS, 2)),
                pltpu.SemaphoreType.DMA((batches, SUBS, 2)),
                pltpu.SemaphoreType.DMA((3,)),
                pltpu.SemaphoreType.DMA((SUBS,)),
            ],
            compiler_params=pltpu.CompilerParams(
                collective_id=0, has_side_effects=True, vmem_limit_bytes=VMEM_LIMIT
            ),
            cost_estimate=pl.CostEstimate(
                flops=flops, bytes_accessed=3 * w_gate.size * 2 + 4 * wire, transcendentals=n * rows * hidden
            ),
            name="mlp_ring",
        )(x, w_gate, w_up, w_down)
        return y

    return jax.shard_map(
        step,
        mesh=mesh,
        in_specs=(P(("dp", "tp"), None), P(None, "tp"), P(None, "tp"), P("tp", None)),
        out_specs=P(("dp", "tp"), None),
        check_vma=False,
    )
```

```python
import functools

import jax
import jax.numpy as jnp
from jax import lax
from jax.experimental import pallas as pl
from jax.experimental.pallas import tpu as pltpu
from jax.sharding import PartitionSpec as P

MESH = pl.DeviceIdType.MESH
VMEM_LIMIT = 61 * 2**20 + 2**19
SUBS = 2


def _kernel(
    n,
    x_ref,
    wg_ref,
    wu_ref,
    wd_ref,
    y_ref,
    xg_ref,
    rs_ref,
    wg,
    wu,
    wd,
    hid,
    xbuf,
    sbuf,
    acc,
    ag_send,
    ag_recv,
    rs_send,
    rs_recv,
    w_sem,
    x_sem,
    r_sem,
):
    rows, _ = x_ref.shape
    hidden = wg.shape[1]
    cols = wd.shape[1]
    half = rows // 2
    piece = half // SUBS
    pair = 2 * piece
    batches = n - 1
    nt_h = 256
    nt_y = 512
    me = lax.axis_index("tp")
    right, left = lax.rem(me + 1, n), lax.rem(me + n - 1, n)

    own = pltpu.make_async_copy(x_ref, xbuf.at[0], x_sem.at[0])
    own.start()
    weights = [
        pltpu.make_async_copy(src, dst, w_sem.at[i])
        for i, (src, dst) in enumerate(((wg_ref, wg), (wu_ref, wu), (wd_ref, wd)))
    ]

    barrier = pltpu.get_barrier_semaphore()
    for neighbour in (left, right):
        pl.semaphore_signal(barrier, inc=1, device_id={"tp": neighbour}, device_id_type=MESH)
    pl.semaphore_wait(barrier, 2)

    def at(s, d):
        return pl.ds(s * pair + d * piece, piece)

    def gather(b, s, d, src):
        return pltpu.make_async_remote_copy(
            src_ref=src,
            dst_ref=xg_ref.at[b, at(s, d)],
            send_sem=ag_send.at[b, s, d],
            recv_sem=ag_recv.at[b, s, d],
            device_id={"tp": right if d == 0 else left},
            device_id_type=MESH,
        )

    def gather_own(b, s, d):
        start = (b if d == 0 else 1 - b) * half + s * piece
        return gather(b, s, d, xbuf.at[0, pl.ds(start, piece)])

    def gather_on(b, s, d):
        return gather(b + 2, s, d, xg_ref.at[b, at(s, d)])

    def home(t, s, d):
        return pl.ds((t if d == 0 else 1 - t) * half + s * piece, piece)

    def reduce(b, s, d, slot, last=False):
        return pltpu.make_async_remote_copy(
            src_ref=sbuf.at[slot, pl.ds(d * piece, piece)],
            dst_ref=y_ref.at[home(0, s, d)] if last else rs_ref.at[b - 1, at(s, d)],
            send_sem=rs_send.at[b, s, d],
            recv_sem=rs_recv.at[b, s, d],
            device_id={"tp": left if d == 0 else right},
            device_id_type=MESH,
        )

    own.wait()
    for b in range(2):
        for s in range(SUBS):
            for d in range(2):
                gather_own(b, s, d).start()
    for w in weights:
        w.start()

    def mlp_in(x_slot, h_slot):
        def step(i, carry):
            c = pl.ds(pl.multiple_of(i * nt_h, nt_h), nt_h)
            x = xbuf[x_slot]
            gate = jnp.dot(x, wg[:, c], preferred_element_type=jnp.float32)
            up = jnp.dot(x, wu[:, c], preferred_element_type=jnp.float32)
            hid[h_slot, :, c] = (jax.nn.silu(gate) * up).astype(jnp.bfloat16)
            return carry

        lax.fori_loop(0, hidden // nt_h, step, 0)

    def x_slot(b):
        return lax.rem(b + 1, 2)

    def x_load(b):
        return pltpu.make_async_copy(xg_ref.at[b], xbuf.at[x_slot(b)], x_sem.at[x_slot(b)])

    def receive(b, forward):
        for s in range(SUBS):
            for d in range(2):
                gather(b, s, d, xg_ref.at[b, at(s, d)]).wait_recv()
                if forward:
                    gather_on(b, s, d).start()

    def batch_in(b):
        x_load(b).wait()
        mlp_in(x_slot(b), b)

    receive(0, True)
    x_load(0).start()
    for w in weights:
        w.wait()
    mlp_in(0, 0)

    def own_term(i, carry):
        c = pl.ds(pl.multiple_of(i * nt_y, nt_y), nt_y)
        acc[:, c] = jnp.dot(hid[0], wd[:, c], preferred_element_type=jnp.float32)
        return carry

    lax.fori_loop(0, cols // nt_y, own_term, 0)

    receive(1, True)
    for b in range(2):
        for s in range(SUBS):
            for d in range(2):
                gather_own(b, s, d).wait_send()
    x_load(1).start()
    batch_in(0)

    def in_only(b, carry):
        receive(b, True)
        x_load(b).start()
        batch_in(b - 1)
        return carry

    lax.fori_loop(2, batches - 2, in_only, 0)
    batch_in(batches - 3)

    def fetch(b, s):
        for d in range(2):
            reduce(b + 2, s, d, 0).wait_recv()
        load(b, s).start()

    def load(b, s):
        r = pl.ds(s * pair, pair)
        return pltpu.make_async_copy(rs_ref.at[b + 1, r], xbuf.at[0, r], r_sem.at[s])

    def batch_out(b, s, slot, add, last=False):
        h = pl.ds(s * pair, pair)
        if add:
            load(b, s).wait()

        def step(i, carry):
            c = pl.ds(pl.multiple_of(i * nt_y, nt_y), nt_y)
            term = jnp.dot(hid[b, h, :], wd[:, c], preferred_element_type=jnp.float32)
            if add:
                term = term + xbuf[0, h, c].astype(jnp.float32)
            sbuf[slot, :, c] = term.astype(jnp.bfloat16)
            return carry

        lax.fori_loop(0, cols // nt_y, step, 0)
        for d in range(2):
            reduce(b, s, d, slot, last).start()

    def in_out(i, carry):
        b = batches - 2 + i
        receive(b, False)
        x_load(b).start()
        batch_in(b)
        for s in range(SUBS):
            batch_out(b, s, i * SUBS + s, False)
        return carry

    lax.fori_loop(0, 2, in_out, 0)

    def order(k):
        return batches - 4 - 2 * (k // 2) + lax.rem(k, 2)

    def out_pair(k, ahead):
        b = order(k)
        for s in range(SUBS):
            if s + 1 < SUBS:
                fetch(b, s + 1)
            elif ahead:
                fetch(order(k + 1), 0)
            slot = lax.rem(k, 2) * SUBS + s
            for d in range(2):
                reduce(b + 2, s, d, slot).wait_send()
            batch_out(b, s, slot, True)

    def out_only(k, carry):
        out_pair(k, True)
        return carry

    fetch(order(0), 0)
    lax.fori_loop(0, batches - 4, out_only, 0)
    out_pair(batches - 4, False)

    for s in range(SUBS):
        for d in range(2):
            reduce(1, s, d, s).wait_recv()
    mine = pltpu.make_async_copy(rs_ref.at[0], xbuf.at[1], x_sem.at[1])
    mine.start()

    for s in range(SUBS):
        for d in range(2):
            reduce(1, s, d, s).wait_send()
        fetch(0, s)
        batch_out(0, s, s, True, last=True)

    mine.wait()
    for s in range(SUBS):
        for d in range(2):
            o = home(1, s, d)
            acc[o, :] = acc[o, :] + xbuf[1, at(s, d), :].astype(jnp.float32)

    for s in range(SUBS):
        for d in range(2):
            for b in range(2, batches):
                gather(b, s, d, xg_ref.at[b, at(s, d)]).wait_send()
            reduce(2, s, d, SUBS + s).wait_send()

    for s in range(SUBS):
        for d in range(2):
            reduce(0, s, d, s, last=True).wait_recv()
        for d in range(2):
            o = home(0, s, d)
            y_ref[o, :] = (acc[o, :] + y_ref[o, :].astype(jnp.float32)).astype(jnp.bfloat16)

    for s in range(SUBS):
        for d in range(2):
            reduce(0, s, d, s, last=True).wait_send()


def solution(mesh):
    n = mesh.shape["tp"]

    def step(x, w_gate, w_up, w_down):
        rows, dim = x.shape
        hidden = w_gate.shape[1]
        batches = n - 1
        piece = rows // (2 * SUBS)
        flops = 6 * n * rows * dim * hidden
        wire = 2 * batches * rows * dim * 2
        any_space = pl.BlockSpec(memory_space=pltpu.MemorySpace.HBM)
        y, _, _ = pl.pallas_call(
            functools.partial(_kernel, n),
            out_shape=(
                pltpu.VMEM((rows, dim), jnp.bfloat16),
                jax.ShapeDtypeStruct((batches, rows, dim), jnp.bfloat16),
                jax.ShapeDtypeStruct((batches - 1, rows, dim), jnp.bfloat16),
            ),
            in_specs=[any_space] * 4,
            out_specs=(pl.BlockSpec(memory_space=pltpu.MemorySpace.VMEM), any_space, any_space),
            scratch_shapes=[
                pltpu.VMEM(w_gate.shape, jnp.bfloat16),
                pltpu.VMEM(w_up.shape, jnp.bfloat16),
                pltpu.VMEM(w_down.shape, jnp.bfloat16),
                pltpu.VMEM((batches, rows, hidden), jnp.bfloat16),
                pltpu.VMEM((2, rows, dim), jnp.bfloat16),
                pltpu.VMEM((2 * SUBS, 2 * piece, dim), jnp.bfloat16),
                pltpu.VMEM((rows, dim), jnp.float32),
                pltpu.SemaphoreType.DMA((batches, SUBS, 2)),
                pltpu.SemaphoreType.DMA((batches, SUBS, 2)),
                pltpu.SemaphoreType.DMA((batches, SUBS, 2)),
                pltpu.SemaphoreType.DMA((batches, SUBS, 2)),
                pltpu.SemaphoreType.DMA((3,)),
                pltpu.SemaphoreType.DMA((2,)),
                pltpu.SemaphoreType.DMA((SUBS,)),
            ],
            compiler_params=pltpu.CompilerParams(
                collective_id=0, has_side_effects=True, vmem_limit_bytes=VMEM_LIMIT
            ),
            cost_estimate=pl.CostEstimate(
                flops=flops, bytes_accessed=3 * w_gate.size * 2 + 4 * wire, transcendentals=n * rows * hidden
            ),
            name="mlp_ring",
        )(x, w_gate, w_up, w_down)
        return y

    return jax.shard_map(
        step,
        mesh=mesh,
        in_specs=(P(("dp", "tp"), None), P(None, "tp"), P(None, "tp"), P("tp", None)),
        out_specs=P(("dp", "tp"), None),
        check_vma=False,
    )
```

```python
import functools

import jax
import jax.numpy as jnp
from jax import lax
from jax.experimental import pallas as pl
from jax.experimental.pallas import tpu as pltpu
from jax.sharding import PartitionSpec as P

MESH = pl.DeviceIdType.MESH
VMEM_LIMIT = 61 * 2**20 + 2**19
SUBS = 2


def _kernel(
    n,
    x_ref,
    wg_ref,
    wu_ref,
    wd_ref,
    y_ref,
    xg_ref,
    rs_ref,
    wg,
    wu,
    wd,
    hid,
    xbuf,
    sbuf,
    acc,
    ag_send,
    ag_recv,
    rs_send,
    rs_recv,
    w_sem,
    x_sem,
    r_sem,
):
    rows, _ = x_ref.shape
    hidden = wg.shape[1]
    cols = wd.shape[1]
    half = rows // 2
    piece = half // SUBS
    pair = 2 * piece
    batches = n - 1
    nt_h = 256
    nt_y = 512
    me = lax.axis_index("tp")
    right, left = lax.rem(me + 1, n), lax.rem(me + n - 1, n)

    own = pltpu.make_async_copy(x_ref, xbuf.at[0], x_sem.at[0])
    weights = [
        pltpu.make_async_copy(src, dst, w_sem.at[i])
        for i, (src, dst) in enumerate(((wg_ref, wg), (wu_ref, wu), (wd_ref, wd)))
    ]

    barrier = pltpu.get_barrier_semaphore()
    for neighbour in (left, right):
        pl.semaphore_signal(barrier, inc=1, device_id={"tp": neighbour}, device_id_type=MESH)
    pl.semaphore_wait(barrier, 2)

    def at(s, d):
        return pl.ds(s * pair + d * piece, piece)

    def gather(b, s, d, src):
        return pltpu.make_async_remote_copy(
            src_ref=src,
            dst_ref=xg_ref.at[b, at(s, d)],
            send_sem=ag_send.at[b, s, d],
            recv_sem=ag_recv.at[b, s, d],
            device_id={"tp": right if d == 0 else left},
            device_id_type=MESH,
        )

    def gather_own(b, s, d):
        start = (b if d == 0 else 1 - b) * half + s * piece
        return gather(b, s, d, x_ref.at[pl.ds(start, piece)])

    def gather_on(b, s, d):
        return gather(b + 2, s, d, xg_ref.at[b, at(s, d)])

    def home(t, s, d):
        return pl.ds((t if d == 0 else 1 - t) * half + s * piece, piece)

    def reduce(b, s, d, slot, last=False):
        return pltpu.make_async_remote_copy(
            src_ref=sbuf.at[slot, pl.ds(d * piece, piece)],
            dst_ref=y_ref.at[home(0, s, d)] if last else rs_ref.at[b - 1, at(s, d)],
            send_sem=rs_send.at[b, s, d],
            recv_sem=rs_recv.at[b, s, d],
            device_id={"tp": left if d == 0 else right},
            device_id_type=MESH,
        )

    for b in range(2):
        for s in range(SUBS):
            for d in range(2):
                gather_own(b, s, d).start()
    own.start()
    for w in weights:
        w.start()

    def mlp_in(x_slot, h_slot):
        def step(i, carry):
            c = pl.ds(pl.multiple_of(i * nt_h, nt_h), nt_h)
            x = xbuf[x_slot]
            gate = jnp.dot(x, wg[:, c], preferred_element_type=jnp.float32)
            up = jnp.dot(x, wu[:, c], preferred_element_type=jnp.float32)
            hid[h_slot, :, c] = (jax.nn.silu(gate) * up).astype(jnp.bfloat16)
            return carry

        lax.fori_loop(0, hidden // nt_h, step, 0)

    def x_slot(b):
        return lax.rem(b + 1, 2)

    def x_load(b):
        return pltpu.make_async_copy(xg_ref.at[b], xbuf.at[x_slot(b)], x_sem.at[x_slot(b)])

    def receive(b, forward):
        for s in range(SUBS):
            for d in range(2):
                gather(b, s, d, xg_ref.at[b, at(s, d)]).wait_recv()
                if forward:
                    gather_on(b, s, d).start()

    def batch_in(b):
        x_load(b).wait()
        mlp_in(x_slot(b), b)

    receive(0, True)
    x_load(0).start()
    own.wait()
    for w in weights:
        w.wait()
    mlp_in(0, 0)

    def own_term(i, carry):
        c = pl.ds(pl.multiple_of(i * nt_y, nt_y), nt_y)
        acc[:, c] = jnp.dot(hid[0], wd[:, c], preferred_element_type=jnp.float32)
        return carry

    lax.fori_loop(0, cols // nt_y, own_term, 0)

    receive(1, True)
    x_load(1).start()
    batch_in(0)

    def in_only(b, carry):
        receive(b, True)
        x_load(b).start()
        batch_in(b - 1)
        return carry

    lax.fori_loop(2, batches - 2, in_only, 0)
    batch_in(batches - 3)

    def fetch(b, s):
        for d in range(2):
            reduce(b + 2, s, d, 0).wait_recv()
        load(b, s).start()

    def load(b, s):
        r = pl.ds(s * pair, pair)
        return pltpu.make_async_copy(rs_ref.at[b + 1, r], xbuf.at[0, r], r_sem.at[s])

    def batch_out(b, s, slot, add, last=False):
        h = pl.ds(s * pair, pair)
        if add:
            load(b, s).wait()

        def step(i, carry):
            c = pl.ds(pl.multiple_of(i * nt_y, nt_y), nt_y)
            term = jnp.dot(hid[b, h, :], wd[:, c], preferred_element_type=jnp.float32)
            if add:
                term = term + xbuf[0, h, c].astype(jnp.float32)
            sbuf[slot, :, c] = term.astype(jnp.bfloat16)
            return carry

        lax.fori_loop(0, cols // nt_y, step, 0)
        for d in range(2):
            reduce(b, s, d, slot, last).start()

    def in_out(i, carry):
        b = batches - 2 + i
        receive(b, False)
        x_load(b).start()
        batch_in(b)
        for s in range(SUBS):
            batch_out(b, s, i * SUBS + s, False)
        return carry

    lax.fori_loop(0, 2, in_out, 0)

    def order(k):
        return batches - 4 - 2 * (k // 2) + lax.rem(k, 2)

    def out_pair(k, ahead):
        b = order(k)
        for s in range(SUBS):
            if s + 1 < SUBS:
                fetch(b, s + 1)
            elif ahead:
                fetch(order(k + 1), 0)
            slot = lax.rem(k, 2) * SUBS + s
            for d in range(2):
                reduce(b + 2, s, d, slot).wait_send()
            batch_out(b, s, slot, True)

    def out_only(k, carry):
        out_pair(k, True)
        return carry

    fetch(order(0), 0)
    lax.fori_loop(0, batches - 4, out_only, 0)
    out_pair(batches - 4, False)

    for s in range(SUBS):
        for d in range(2):
            reduce(1, s, d, s).wait_recv()
    mine = pltpu.make_async_copy(rs_ref.at[0], xbuf.at[1], x_sem.at[1])
    mine.start()

    for s in range(SUBS):
        for d in range(2):
            reduce(1, s, d, s).wait_send()
        fetch(0, s)
        batch_out(0, s, s, True, last=True)

    mine.wait()
    for s in range(SUBS):
        for d in range(2):
            o = home(1, s, d)
            acc[o, :] = acc[o, :] + xbuf[1, at(s, d), :].astype(jnp.float32)

    for s in range(SUBS):
        for d in range(2):
            for b in range(batches):
                gather(b, s, d, xg_ref.at[b, at(s, d)]).wait_send()
            reduce(2, s, d, SUBS + s).wait_send()

    for s in range(SUBS):
        for d in range(2):
            reduce(0, s, d, s, last=True).wait_recv()
        for d in range(2):
            o = home(0, s, d)
            y_ref[o, :] = (acc[o, :] + y_ref[o, :].astype(jnp.float32)).astype(jnp.bfloat16)

    for s in range(SUBS):
        for d in range(2):
            reduce(0, s, d, s, last=True).wait_send()


def solution(mesh):
    n = mesh.shape["tp"]

    def step(x, w_gate, w_up, w_down):
        rows, dim = x.shape
        hidden = w_gate.shape[1]
        batches = n - 1
        piece = rows // (2 * SUBS)
        flops = 6 * n * rows * dim * hidden
        wire = 2 * batches * rows * dim * 2
        any_space = pl.BlockSpec(memory_space=pltpu.MemorySpace.HBM)
        y, _, _ = pl.pallas_call(
            functools.partial(_kernel, n),
            out_shape=(
                pltpu.VMEM((rows, dim), jnp.bfloat16),
                jax.ShapeDtypeStruct((batches, rows, dim), jnp.bfloat16),
                jax.ShapeDtypeStruct((batches - 1, rows, dim), jnp.bfloat16),
            ),
            in_specs=[any_space] * 4,
            out_specs=(pl.BlockSpec(memory_space=pltpu.MemorySpace.VMEM), any_space, any_space),
            scratch_shapes=[
                pltpu.VMEM(w_gate.shape, jnp.bfloat16),
                pltpu.VMEM(w_up.shape, jnp.bfloat16),
                pltpu.VMEM(w_down.shape, jnp.bfloat16),
                pltpu.VMEM((batches, rows, hidden), jnp.bfloat16),
                pltpu.VMEM((2, rows, dim), jnp.bfloat16),
                pltpu.VMEM((2 * SUBS, 2 * piece, dim), jnp.bfloat16),
                pltpu.VMEM((rows, dim), jnp.float32),
                pltpu.SemaphoreType.DMA((batches, SUBS, 2)),
                pltpu.SemaphoreType.DMA((batches, SUBS, 2)),
                pltpu.SemaphoreType.DMA((batches, SUBS, 2)),
                pltpu.SemaphoreType.DMA((batches, SUBS, 2)),
                pltpu.SemaphoreType.DMA((3,)),
                pltpu.SemaphoreType.DMA((2,)),
                pltpu.SemaphoreType.DMA((SUBS,)),
            ],
            compiler_params=pltpu.CompilerParams(
                collective_id=0, has_side_effects=True, vmem_limit_bytes=VMEM_LIMIT
            ),
            cost_estimate=pl.CostEstimate(
                flops=flops, bytes_accessed=3 * w_gate.size * 2 + 4 * wire, transcendentals=n * rows * hidden
            ),
            name="mlp_ring",
        )(x, w_gate, w_up, w_down)
        return y

    return jax.shard_map(
        step,
        mesh=mesh,
        in_specs=(P(("dp", "tp"), None), P(None, "tp"), P(None, "tp"), P("tp", None)),
        out_specs=P(("dp", "tp"), None),
        check_vma=False,
    )
```

```python
import functools

import jax
import jax.numpy as jnp
from jax import lax
from jax.experimental import pallas as pl
from jax.experimental.pallas import tpu as pltpu
from jax.sharding import PartitionSpec as P

MESH = pl.DeviceIdType.MESH
VMEM_LIMIT = 61 * 2**20 + 2**19
SUBS = 2


def _kernel(
    n,
    x_ref,
    wg_ref,
    wu_ref,
    wd_ref,
    y_ref,
    xg_ref,
    rs_ref,
    wg,
    wu,
    wd,
    hid,
    xbuf,
    sbuf,
    acc,
    ag_send,
    ag_recv,
    rs_send,
    rs_recv,
    w_sem,
    x_sem,
    r_sem,
    ready,
):
    rows, _ = x_ref.shape
    hidden = wg.shape[1]
    cols = wd.shape[1]
    half = rows // 2
    piece = half // SUBS
    pair = 2 * piece
    batches = n - 1
    nt_h = 256
    nt_y = 512
    me = lax.axis_index("tp")
    right, left = lax.rem(me + 1, n), lax.rem(me + n - 1, n)

    own = pltpu.make_async_copy(x_ref, xbuf.at[0], x_sem.at[0])
    weights = [
        pltpu.make_async_copy(src, dst, w_sem.at[i])
        for i, (src, dst) in enumerate(((wg_ref, wg), (wu_ref, wu), (wd_ref, wd)))
    ]

    barrier = pltpu.get_barrier_semaphore()
    pl.semaphore_signal(barrier, inc=1, device_id={"tp": left}, device_id_type=MESH)
    pl.semaphore_wait(barrier, 1)
    pl.semaphore_signal(ready, inc=1, device_id={"tp": right}, device_id_type=MESH)

    def at(s, d):
        return pl.ds(s * pair + d * piece, piece)

    def gather(b, s, d, src):
        return pltpu.make_async_remote_copy(
            src_ref=src,
            dst_ref=xg_ref.at[b, at(s, d)],
            send_sem=ag_send.at[b, s, d],
            recv_sem=ag_recv.at[b, s, d],
            device_id={"tp": right if d == 0 else left},
            device_id_type=MESH,
        )

    def gather_own(b, s, d):
        start = (b if d == 0 else 1 - b) * half + s * piece
        return gather(b, s, d, x_ref.at[pl.ds(start, piece)])

    def gather_on(b, s, d):
        return gather(b + 2, s, d, xg_ref.at[b, at(s, d)])

    def home(t, s, d):
        return pl.ds((t if d == 0 else 1 - t) * half + s * piece, piece)

    def reduce(b, s, d, slot, last=False):
        return pltpu.make_async_remote_copy(
            src_ref=sbuf.at[slot, pl.ds(d * piece, piece)],
            dst_ref=y_ref.at[home(0, s, d)] if last else rs_ref.at[b - 1, at(s, d)],
            send_sem=rs_send.at[b, s, d],
            recv_sem=rs_recv.at[b, s, d],
            device_id={"tp": left if d == 0 else right},
            device_id_type=MESH,
        )

    for d in range(2):
        if d == 1:
            pl.semaphore_wait(ready, 1)
        for b in range(2):
            for s in range(SUBS):
                gather_own(b, s, d).start()
    own.start()
    for w in weights:
        w.start()

    def mlp_in(x_slot, h_slot):
        def step(i, carry):
            c = pl.ds(pl.multiple_of(i * nt_h, nt_h), nt_h)
            x = xbuf[x_slot]
            gate = jnp.dot(x, wg[:, c], preferred_element_type=jnp.float32)
            up = jnp.dot(x, wu[:, c], preferred_element_type=jnp.float32)
            hid[h_slot, :, c] = (jax.nn.silu(gate) * up).astype(jnp.bfloat16)
            return carry

        lax.fori_loop(0, hidden // nt_h, step, 0)

    def x_slot(b):
        return lax.rem(b + 1, 2)

    def x_load(b):
        return pltpu.make_async_copy(xg_ref.at[b], xbuf.at[x_slot(b)], x_sem.at[x_slot(b)])

    def receive(b, forward):
        for s in range(SUBS):
            for d in range(2):
                gather(b, s, d, xg_ref.at[b, at(s, d)]).wait_recv()
                if forward:
                    gather_on(b, s, d).start()

    def batch_in(b):
        x_load(b).wait()
        mlp_in(x_slot(b), b)

    receive(0, True)
    x_load(0).start()
    own.wait()
    for w in weights:
        w.wait()
    mlp_in(0, 0)

    def own_term(i, carry):
        c = pl.ds(pl.multiple_of(i * nt_y, nt_y), nt_y)
        acc[:, c] = jnp.dot(hid[0], wd[:, c], preferred_element_type=jnp.float32)
        return carry

    lax.fori_loop(0, cols // nt_y, own_term, 0)

    receive(1, True)
    x_load(1).start()
    batch_in(0)

    def in_only(b, carry):
        receive(b, True)
        x_load(b).start()
        batch_in(b - 1)
        return carry

    lax.fori_loop(2, batches - 2, in_only, 0)
    batch_in(batches - 3)

    def fetch(b, s):
        for d in range(2):
            reduce(b + 2, s, d, 0).wait_recv()
        load(b, s).start()

    def load(b, s):
        r = pl.ds(s * pair, pair)
        return pltpu.make_async_copy(rs_ref.at[b + 1, r], xbuf.at[0, r], r_sem.at[s])

    def batch_out(b, s, slot, add, last=False):
        h = pl.ds(s * pair, pair)
        if add:
            load(b, s).wait()

        def step(i, carry):
            c = pl.ds(pl.multiple_of(i * nt_y, nt_y), nt_y)
            term = jnp.dot(hid[b, h, :], wd[:, c], preferred_element_type=jnp.float32)
            if add:
                term = term + xbuf[0, h, c].astype(jnp.float32)
            sbuf[slot, :, c] = term.astype(jnp.bfloat16)
            return carry

        lax.fori_loop(0, cols // nt_y, step, 0)
        for d in range(2):
            reduce(b, s, d, slot, last).start()

    def in_out(i, carry):
        b = batches - 2 + i
        receive(b, False)
        x_load(b).start()
        batch_in(b)
        for s in range(SUBS):
            batch_out(b, s, i * SUBS + s, False)
        return carry

    lax.fori_loop(0, 2, in_out, 0)

    def order(k):
        return batches - 4 - 2 * (k // 2) + lax.rem(k, 2)

    def out_pair(k, ahead):
        b = order(k)
        for s in range(SUBS):
            if s + 1 < SUBS:
                fetch(b, s + 1)
            elif ahead:
                fetch(order(k + 1), 0)
            slot = lax.rem(k, 2) * SUBS + s
            for d in range(2):
                reduce(b + 2, s, d, slot).wait_send()
            batch_out(b, s, slot, True)

    def out_only(k, carry):
        out_pair(k, True)
        return carry

    fetch(order(0), 0)
    lax.fori_loop(0, batches - 4, out_only, 0)
    out_pair(batches - 4, False)

    for s in range(SUBS):
        for d in range(2):
            reduce(1, s, d, s).wait_recv()
    mine = pltpu.make_async_copy(rs_ref.at[0], xbuf.at[1], x_sem.at[1])
    mine.start()

    for s in range(SUBS):
        for d in range(2):
            reduce(1, s, d, s).wait_send()
        fetch(0, s)
        batch_out(0, s, s, True, last=True)

    mine.wait()
    for s in range(SUBS):
        for d in range(2):
            o = home(1, s, d)
            acc[o, :] = acc[o, :] + xbuf[1, at(s, d), :].astype(jnp.float32)

    for s in range(SUBS):
        for d in range(2):
            for b in range(batches):
                gather(b, s, d, xg_ref.at[b, at(s, d)]).wait_send()
            reduce(2, s, d, SUBS + s).wait_send()

    for s in range(SUBS):
        for d in range(2):
            reduce(0, s, d, s, last=True).wait_recv()
        for d in range(2):
            o = home(0, s, d)
            y_ref[o, :] = (acc[o, :] + y_ref[o, :].astype(jnp.float32)).astype(jnp.bfloat16)

    for s in range(SUBS):
        for d in range(2):
            reduce(0, s, d, s, last=True).wait_send()


def solution(mesh):
    n = mesh.shape["tp"]

    def step(x, w_gate, w_up, w_down):
        rows, dim = x.shape
        hidden = w_gate.shape[1]
        batches = n - 1
        piece = rows // (2 * SUBS)
        flops = 6 * n * rows * dim * hidden
        wire = 2 * batches * rows * dim * 2
        any_space = pl.BlockSpec(memory_space=pltpu.MemorySpace.HBM)
        y, _, _ = pl.pallas_call(
            functools.partial(_kernel, n),
            out_shape=(
                pltpu.VMEM((rows, dim), jnp.bfloat16),
                jax.ShapeDtypeStruct((batches, rows, dim), jnp.bfloat16),
                jax.ShapeDtypeStruct((batches - 1, rows, dim), jnp.bfloat16),
            ),
            in_specs=[any_space] * 4,
            out_specs=(pl.BlockSpec(memory_space=pltpu.MemorySpace.VMEM), any_space, any_space),
            scratch_shapes=[
                pltpu.VMEM(w_gate.shape, jnp.bfloat16),
                pltpu.VMEM(w_up.shape, jnp.bfloat16),
                pltpu.VMEM(w_down.shape, jnp.bfloat16),
                pltpu.VMEM((batches, rows, hidden), jnp.bfloat16),
                pltpu.VMEM((2, rows, dim), jnp.bfloat16),
                pltpu.VMEM((2 * SUBS, 2 * piece, dim), jnp.bfloat16),
                pltpu.VMEM((rows, dim), jnp.float32),
                pltpu.SemaphoreType.DMA((batches, SUBS, 2)),
                pltpu.SemaphoreType.DMA((batches, SUBS, 2)),
                pltpu.SemaphoreType.DMA((batches, SUBS, 2)),
                pltpu.SemaphoreType.DMA((batches, SUBS, 2)),
                pltpu.SemaphoreType.DMA((3,)),
                pltpu.SemaphoreType.DMA((2,)),
                pltpu.SemaphoreType.DMA((SUBS,)),
                pltpu.SemaphoreType.REGULAR,
            ],
            compiler_params=pltpu.CompilerParams(
                collective_id=0, has_side_effects=True, vmem_limit_bytes=VMEM_LIMIT
            ),
            cost_estimate=pl.CostEstimate(
                flops=flops, bytes_accessed=3 * w_gate.size * 2 + 4 * wire, transcendentals=n * rows * hidden
            ),
            name="mlp_ring",
        )(x, w_gate, w_up, w_down)
        return y

    return jax.shard_map(
        step,
        mesh=mesh,
        in_specs=(P(("dp", "tp"), None), P(None, "tp"), P(None, "tp"), P("tp", None)),
        out_specs=P(("dp", "tp"), None),
        check_vma=False,
    )
```

```python
import functools

import jax
import jax.numpy as jnp
from jax import lax
from jax.experimental import pallas as pl
from jax.experimental.pallas import tpu as pltpu
from jax.sharding import PartitionSpec as P

MESH = pl.DeviceIdType.MESH
VMEM_LIMIT = 61 * 2**20 + 2**19
SUBS = 2


def _kernel(
    n,
    x_ref,
    wg_ref,
    wu_ref,
    wd_ref,
    y_ref,
    xg_ref,
    rs_ref,
    wg,
    wu,
    wd,
    hid,
    xbuf,
    sbuf,
    acc,
    ag_send,
    ag_recv,
    rs_send,
    rs_recv,
    w_sem,
    x_sem,
    r_sem,
    ready,
):
    rows, _ = x_ref.shape
    hidden = wg.shape[1]
    cols = wd.shape[1]
    half = rows // 2
    piece = half // SUBS
    pair = 2 * piece
    batches = n - 1
    nt_h = 256
    nt_y = 512
    me = lax.axis_index("tp")
    right, left = lax.rem(me + 1, n), lax.rem(me + n - 1, n)

    own = pltpu.make_async_copy(x_ref, xbuf.at[0], x_sem.at[0])
    weights = [
        pltpu.make_async_copy(src, dst, w_sem.at[i])
        for i, (src, dst) in enumerate(((wg_ref, wg), (wu_ref, wu), (wd_ref, wd)))
    ]

    barrier = pltpu.get_barrier_semaphore()
    pl.semaphore_signal(barrier, inc=1, device_id={"tp": left}, device_id_type=MESH)
    pl.semaphore_wait(barrier, 1)
    pl.semaphore_signal(ready, inc=1, device_id={"tp": right}, device_id_type=MESH)

    def at(s, d):
        return pl.ds(s * pair + d * piece, piece)

    def gather(b, s, d, src):
        return pltpu.make_async_remote_copy(
            src_ref=src,
            dst_ref=xg_ref.at[b, at(s, d)],
            send_sem=ag_send.at[b, s, d],
            recv_sem=ag_recv.at[b, s, d],
            device_id={"tp": right if d == 0 else left},
            device_id_type=MESH,
        )

    def gather_own(b, s, d):
        start = (b if d == 0 else 1 - b) * half + s * piece
        return gather(b, s, d, x_ref.at[pl.ds(start, piece)])

    def gather_on(b, s, d):
        return gather(b + 2, s, d, xg_ref.at[b, at(s, d)])

    def home(t, s, d):
        return pl.ds((t if d == 0 else 1 - t) * half + s * piece, piece)

    def reduce(b, s, d, slot, last=False):
        return pltpu.make_async_remote_copy(
            src_ref=sbuf.at[slot, pl.ds(d * piece, piece)],
            dst_ref=y_ref.at[home(0, s, d)] if last else rs_ref.at[b - 1, at(s, d)],
            send_sem=rs_send.at[b, s, d],
            recv_sem=rs_recv.at[b, s, d],
            device_id={"tp": left if d == 0 else right},
            device_id_type=MESH,
        )

    for d in range(2):
        if d == 1:
            pl.semaphore_wait(ready, 1)
        for b in range(2):
            for s in range(SUBS):
                gather_own(b, s, d).start()
    own.start()
    for w in weights:
        w.start()

    def mlp_in(x_slot, h_slot):
        def step(i, carry):
            c = pl.ds(pl.multiple_of(i * nt_h, nt_h), nt_h)
            x = xbuf[x_slot]
            gate = jnp.dot(x, wg[:, c], preferred_element_type=jnp.float32)
            up = jnp.dot(x, wu[:, c], preferred_element_type=jnp.float32)
            hid[h_slot, :, c] = (jax.nn.silu(gate) * up).astype(jnp.bfloat16)
            return carry

        lax.fori_loop(0, hidden // nt_h, step, 0)

    def x_slot(b):
        return lax.rem(b + 1, 2)

    def x_load(b):
        return pltpu.make_async_copy(xg_ref.at[b], xbuf.at[x_slot(b)], x_sem.at[x_slot(b)])

    def receive(b, forward):
        for s in range(SUBS):
            for d in range(2):
                gather(b, s, d, xg_ref.at[b, at(s, d)]).wait_recv()
                if forward:
                    gather_on(b, s, d).start()

    def batch_in(b):
        x_load(b).wait()
        mlp_in(x_slot(b), b)

    receive(0, True)
    x_load(0).start()
    own.wait()
    for w in weights:
        w.wait()
    mlp_in(0, 0)

    def own_term(i, carry):
        c = pl.ds(pl.multiple_of(i * nt_y, nt_y), nt_y)
        acc[:, c] = jnp.dot(hid[0], wd[:, c], preferred_element_type=jnp.float32)
        return carry

    lax.fori_loop(0, cols // nt_y, own_term, 0)

    receive(1, True)
    x_load(1).start()
    batch_in(0)

    def in_only(b, carry):
        receive(b, True)
        x_load(b).start()
        batch_in(b - 1)
        return carry

    lax.fori_loop(2, batches - 2, in_only, 0)
    batch_in(batches - 3)

    def load(b, s, p):
        r = pl.ds(s * pair, pair)
        return pltpu.make_async_copy(rs_ref.at[b + 1, r], xbuf.at[0, pl.ds(p * pair, pair)], r_sem.at[p])

    def fetch(b, s, p):
        for d in range(2):
            reduce(b + 2, s, d, 0).wait_recv()
        load(b, s, p).start()

    def batch_out(b, s, slot, p=None, last=False):
        h = pl.ds(s * pair, pair)
        if p is not None:
            load(b, s, p).wait()

        def step(i, carry):
            c = pl.ds(pl.multiple_of(i * nt_y, nt_y), nt_y)
            term = jnp.dot(hid[b, h, :], wd[:, c], preferred_element_type=jnp.float32)
            if p is not None:
                term = term + xbuf[0, p * pair : (p + 1) * pair, c].astype(jnp.float32)
            sbuf[slot, :, c] = term.astype(jnp.bfloat16)
            return carry

        lax.fori_loop(0, cols // nt_y, step, 0)
        for d in range(2):
            reduce(b, s, d, slot, last).start()

    def in_out(i, carry):
        b = batches - 2 + i
        receive(b, False)
        x_load(b).start()
        batch_in(b)
        for s in range(SUBS):
            batch_out(b, s, i * SUBS + s)
        return carry

    lax.fori_loop(0, 2, in_out, 0)

    order = [(b, s) for b in (batches - 2, batches - 1) for s in range(SUBS)]
    for r in range(n // 2 - 2, 0, -1):
        two = (2 * r - 1, 2 * r) if r == n // 2 - 2 else (2 * r, 2 * r - 1)
        order += [(b, s) for s in range(SUBS) for b in two]
    order += [(0, s) for s in range(SUBS)]
    slots = 2 * SUBS
    mine = pltpu.make_async_copy(rs_ref.at[0], xbuf.at[1], x_sem.at[1])

    def back(k):
        b, s = order[k]
        return k - order.index((b + 2, s))

    fetched = -1
    for k in range(slots, len(order)):
        b, s = order[k]
        if fetched < k:
            fetch(b, s, k % 2)
            fetched = k
        if k + 1 < len(order) and back(k + 1) >= slots:
            fetch(*order[k + 1], (k + 1) % 2)
            fetched = k + 1
        for d in range(2):
            reduce(*order[k - slots], d, k % slots).wait_send()
        batch_out(b, s, k % slots, k % 2, last=b == 0)

    for s in range(SUBS):
        for d in range(2):
            reduce(1, s, d, s).wait_recv()
    mine.start()
    mine.wait()
    for s in range(SUBS):
        for d in range(2):
            o = home(1, s, d)
            acc[o, :] = acc[o, :] + xbuf[1, at(s, d), :].astype(jnp.float32)

    for s in range(SUBS):
        for d in range(2):
            for b in range(batches):
                gather(b, s, d, xg_ref.at[b, at(s, d)]).wait_send()
    for k in range(len(order) - slots, len(order) - SUBS):
        for d in range(2):
            reduce(*order[k], d, k % slots).wait_send()

    for s in range(SUBS):
        for d in range(2):
            reduce(0, s, d, s, last=True).wait_recv()
        for d in range(2):
            o = home(0, s, d)
            y_ref[o, :] = (acc[o, :] + y_ref[o, :].astype(jnp.float32)).astype(jnp.bfloat16)

    for s in range(SUBS):
        for d in range(2):
            reduce(0, s, d, s, last=True).wait_send()


def solution(mesh):
    n = mesh.shape["tp"]

    def step(x, w_gate, w_up, w_down):
        rows, dim = x.shape
        hidden = w_gate.shape[1]
        batches = n - 1
        piece = rows // (2 * SUBS)
        flops = 6 * n * rows * dim * hidden
        wire = 2 * batches * rows * dim * 2
        any_space = pl.BlockSpec(memory_space=pltpu.MemorySpace.HBM)
        y, _, _ = pl.pallas_call(
            functools.partial(_kernel, n),
            out_shape=(
                pltpu.VMEM((rows, dim), jnp.bfloat16),
                jax.ShapeDtypeStruct((batches, rows, dim), jnp.bfloat16),
                jax.ShapeDtypeStruct((batches - 1, rows, dim), jnp.bfloat16),
            ),
            in_specs=[any_space] * 4,
            out_specs=(pl.BlockSpec(memory_space=pltpu.MemorySpace.VMEM), any_space, any_space),
            scratch_shapes=[
                pltpu.VMEM(w_gate.shape, jnp.bfloat16),
                pltpu.VMEM(w_up.shape, jnp.bfloat16),
                pltpu.VMEM(w_down.shape, jnp.bfloat16),
                pltpu.VMEM((batches, rows, hidden), jnp.bfloat16),
                pltpu.VMEM((2, rows, dim), jnp.bfloat16),
                pltpu.VMEM((2 * SUBS, 2 * piece, dim), jnp.bfloat16),
                pltpu.VMEM((rows, dim), jnp.float32),
                pltpu.SemaphoreType.DMA((batches, SUBS, 2)),
                pltpu.SemaphoreType.DMA((batches, SUBS, 2)),
                pltpu.SemaphoreType.DMA((batches, SUBS, 2)),
                pltpu.SemaphoreType.DMA((batches, SUBS, 2)),
                pltpu.SemaphoreType.DMA((3,)),
                pltpu.SemaphoreType.DMA((2,)),
                pltpu.SemaphoreType.DMA((SUBS,)),
                pltpu.SemaphoreType.REGULAR,
            ],
            compiler_params=pltpu.CompilerParams(
                collective_id=0, has_side_effects=True, vmem_limit_bytes=VMEM_LIMIT
            ),
            cost_estimate=pl.CostEstimate(
                flops=flops, bytes_accessed=3 * w_gate.size * 2 + 4 * wire, transcendentals=n * rows * hidden
            ),
            name="mlp_ring",
        )(x, w_gate, w_up, w_down)
        return y

    return jax.shard_map(
        step,
        mesh=mesh,
        in_specs=(P(("dp", "tp"), None), P(None, "tp"), P(None, "tp"), P("tp", None)),
        out_specs=P(("dp", "tp"), None),
        check_vma=False,
    )
```

```python
import functools

import jax
import jax.numpy as jnp
from jax import lax
from jax.experimental import pallas as pl
from jax.experimental.pallas import tpu as pltpu
from jax.sharding import PartitionSpec as P

MESH = pl.DeviceIdType.MESH
VMEM_LIMIT = 57 * 2**20 + 2**19
SUBS = 2


def _kernel(
    n,
    x_ref,
    wg_ref,
    wu_ref,
    wd_ref,
    acc,
    y_ref,
    xg_ref,
    rs_ref,
    wg,
    wu,
    wd,
    hid,
    xbuf,
    sbuf,
    ag_send,
    ag_recv,
    rs_send,
    rs_recv,
    w_sem,
    x_sem,
    r_sem,
    ready,
):
    rows, _ = x_ref.shape
    hidden = wg.shape[1]
    cols = wd.shape[1]
    half = rows // 2
    piece = half // SUBS
    pair = 2 * piece
    batches = n - 1
    nt_h = 256
    nt_y = 512
    me = lax.axis_index("tp")
    right, left = lax.rem(me + 1, n), lax.rem(me + n - 1, n)

    own = pltpu.make_async_copy(x_ref, xbuf.at[0], x_sem.at[0])
    weights = [
        pltpu.make_async_copy(src, dst, w_sem.at[i])
        for i, (src, dst) in enumerate(((wg_ref, wg), (wu_ref, wu), (wd_ref, wd)))
    ]

    barrier = pltpu.get_barrier_semaphore()
    pl.semaphore_signal(barrier, inc=1, device_id={"tp": left}, device_id_type=MESH)
    pl.semaphore_wait(barrier, 1)
    pl.semaphore_signal(ready, inc=1, device_id={"tp": right}, device_id_type=MESH)

    def at(s, d):
        return pl.ds(s * pair + d * piece, piece)

    def gather(b, s, d, src):
        return pltpu.make_async_remote_copy(
            src_ref=src,
            dst_ref=xg_ref.at[b, at(s, d)],
            send_sem=ag_send.at[b, s, d],
            recv_sem=ag_recv.at[b, s, d],
            device_id={"tp": right if d == 0 else left},
            device_id_type=MESH,
        )

    def gather_own(b, s, d):
        start = (b if d == 0 else 1 - b) * half + s * piece
        return gather(b, s, d, x_ref.at[pl.ds(start, piece)])

    def gather_on(b, s, d):
        return gather(b + 2, s, d, xg_ref.at[b, at(s, d)])

    def home(t, s, d):
        return pl.ds((t if d == 0 else 1 - t) * half + s * piece, piece)

    def reduce(b, s, d, slot, last=False):
        return pltpu.make_async_remote_copy(
            src_ref=sbuf.at[slot, pl.ds(d * piece, piece)],
            dst_ref=y_ref.at[home(0, s, d)] if last else rs_ref.at[b - 1, at(s, d)],
            send_sem=rs_send.at[b, s, d],
            recv_sem=rs_recv.at[b, s, d],
            device_id={"tp": left if d == 0 else right},
            device_id_type=MESH,
        )

    for d in range(2):
        if d == 1:
            pl.semaphore_wait(ready, 1)
        for b in range(2):
            for s in range(SUBS):
                gather_own(b, s, d).start()
    own.start()
    for w in weights:
        w.start()

    def mlp_in(x_slot, h_slot):
        def step(i, carry):
            c = pl.ds(pl.multiple_of(i * nt_h, nt_h), nt_h)
            x = xbuf[x_slot]
            gate = jnp.dot(x, wg[:, c], preferred_element_type=jnp.float32)
            up = jnp.dot(x, wu[:, c], preferred_element_type=jnp.float32)
            hid[h_slot, :, c] = (jax.nn.silu(gate) * up).astype(jnp.bfloat16)
            return carry

        lax.fori_loop(0, hidden // nt_h, step, 0)

    def x_slot(b):
        return lax.rem(b + 1, 2)

    def x_load(b):
        return pltpu.make_async_copy(xg_ref.at[b], xbuf.at[x_slot(b)], x_sem.at[x_slot(b)])

    def receive(b, forward):
        for s in range(SUBS):
            for d in range(2):
                gather(b, s, d, xg_ref.at[b, at(s, d)]).wait_recv()
                if forward:
                    gather_on(b, s, d).start()

    def batch_in(b):
        x_load(b).wait()
        mlp_in(x_slot(b), b)

    receive(0, True)
    x_load(0).start()
    own.wait()
    for w in weights:
        w.wait()
    mlp_in(0, 0)

    def own_term(i, carry):
        c = pl.ds(pl.multiple_of(i * nt_y, nt_y), nt_y)
        acc[:, c] = jnp.dot(hid[0], wd[:, c], preferred_element_type=jnp.float32)
        return carry

    lax.fori_loop(0, cols // nt_y, own_term, 0)

    receive(1, True)
    x_load(1).start()
    batch_in(0)

    def in_only(b, carry):
        receive(b, True)
        x_load(b).start()
        batch_in(b - 1)
        return carry

    lax.fori_loop(2, batches - 2, in_only, 0)
    batch_in(batches - 3)

    def fetch(b, s):
        for d in range(2):
            reduce(b + 2, s, d, 0).wait_recv()
        load(b, s).start()

    def load(b, s):
        r = pl.ds(s * pair, pair)
        return pltpu.make_async_copy(rs_ref.at[b + 1, r], xbuf.at[0, r], r_sem.at[s])

    def batch_out(b, s, slot, add, last=False):
        h = pl.ds(s * pair, pair)
        if add:
            load(b, s).wait()

        def step(i, carry):
            c = pl.ds(pl.multiple_of(i * nt_y, nt_y), nt_y)
            term = jnp.dot(hid[b, h, :], wd[:, c], preferred_element_type=jnp.float32)
            if add:
                term = term + xbuf[0, h, c].astype(jnp.float32)
            sbuf[slot, :, c] = term.astype(jnp.bfloat16)
            return carry

        lax.fori_loop(0, cols // nt_y, step, 0)
        for d in range(2):
            reduce(b, s, d, slot, last).start()

    def in_out(i, carry):
        b = batches - 2 + i
        receive(b, False)
        x_load(b).start()
        batch_in(b)
        for s in range(SUBS):
            batch_out(b, s, i * SUBS + s, False)
        return carry

    lax.fori_loop(0, 2, in_out, 0)

    def order(k):
        return batches - 4 - 2 * (k // 2) + lax.rem(k, 2)

    def out_pair(k, ahead):
        b = order(k)
        for s in range(SUBS):
            if s + 1 < SUBS:
                fetch(b, s + 1)
            elif ahead:
                fetch(order(k + 1), 0)
            slot = lax.rem(k, 2) * SUBS + s
            for d in range(2):
                reduce(b + 2, s, d, slot).wait_send()
            batch_out(b, s, slot, True)

    def out_only(k, carry):
        out_pair(k, True)
        return carry

    fetch(order(0), 0)
    lax.fori_loop(0, batches - 4, out_only, 0)
    out_pair(batches - 4, False)

    for s in range(SUBS):
        for d in range(2):
            reduce(1, s, d, s).wait_recv()
    mine = pltpu.make_async_copy(rs_ref.at[0], xbuf.at[1], x_sem.at[1])
    mine.start()

    for s in range(SUBS):
        for d in range(2):
            reduce(1, s, d, s).wait_send()
        fetch(0, s)
        batch_out(0, s, s, True, last=True)

    mine.wait()
    for s in range(SUBS):
        for d in range(2):
            o = home(1, s, d)
            acc[o, :] = acc[o, :] + xbuf[1, at(s, d), :].astype(jnp.float32)

    for s in range(SUBS):
        for d in range(2):
            for b in range(batches):
                gather(b, s, d, xg_ref.at[b, at(s, d)]).wait_send()
            reduce(2, s, d, SUBS + s).wait_send()

    for s in range(SUBS):
        for d in range(2):
            reduce(0, s, d, s, last=True).wait_recv()
            reduce(0, s, d, s, last=True).wait_send()


def solution(mesh):
    n = mesh.shape["tp"]

    def step(x, w_gate, w_up, w_down):
        rows, dim = x.shape
        hidden = w_gate.shape[1]
        batches = n - 1
        piece = rows // (2 * SUBS)
        flops = 6 * n * rows * dim * hidden
        wire = 2 * batches * rows * dim * 2
        vmem_space = pl.BlockSpec(memory_space=pltpu.MemorySpace.VMEM)
        any_space = pl.BlockSpec(memory_space=pltpu.MemorySpace.HBM)
        total, last, _, _ = pl.pallas_call(
            functools.partial(_kernel, n),
            out_shape=(
                pltpu.VMEM((rows, dim), jnp.float32),
                pltpu.VMEM((rows, dim), jnp.bfloat16),
                jax.ShapeDtypeStruct((batches, rows, dim), jnp.bfloat16),
                jax.ShapeDtypeStruct((batches - 1, rows, dim), jnp.bfloat16),
            ),
            in_specs=[any_space] * 4,
            out_specs=(vmem_space, vmem_space, any_space, any_space),
            scratch_shapes=[
                pltpu.VMEM(w_gate.shape, jnp.bfloat16),
                pltpu.VMEM(w_up.shape, jnp.bfloat16),
                pltpu.VMEM(w_down.shape, jnp.bfloat16),
                pltpu.VMEM((batches, rows, hidden), jnp.bfloat16),
                pltpu.VMEM((2, rows, dim), jnp.bfloat16),
                pltpu.VMEM((2 * SUBS, 2 * piece, dim), jnp.bfloat16),
                pltpu.SemaphoreType.DMA((batches, SUBS, 2)),
                pltpu.SemaphoreType.DMA((batches, SUBS, 2)),
                pltpu.SemaphoreType.DMA((batches, SUBS, 2)),
                pltpu.SemaphoreType.DMA((batches, SUBS, 2)),
                pltpu.SemaphoreType.DMA((3,)),
                pltpu.SemaphoreType.DMA((2,)),
                pltpu.SemaphoreType.DMA((SUBS,)),
                pltpu.SemaphoreType.REGULAR,
            ],
            compiler_params=pltpu.CompilerParams(
                collective_id=0, has_side_effects=True, vmem_limit_bytes=VMEM_LIMIT
            ),
            cost_estimate=pl.CostEstimate(
                flops=flops, bytes_accessed=3 * w_gate.size * 2 + 4 * wire, transcendentals=n * rows * hidden
            ),
            name="mlp_ring",
        )(x, w_gate, w_up, w_down)
        return (total + last.astype(jnp.float32)).astype(jnp.bfloat16)

    return jax.shard_map(
        step,
        mesh=mesh,
        in_specs=(P(("dp", "tp"), None), P(None, "tp"), P(None, "tp"), P("tp", None)),
        out_specs=P(("dp", "tp"), None),
        check_vma=False,
    )
```
